32 devices in a mesh: gx: 4 (over z), gy: 8 (over y, x, core).
Axes of the slice: x: 2, y: 2, z: 4, core: 2. Of those that a mesh axis runs over, the one named last changes fastest.
Arguments:
- state_prev: float32 [128, 128, 512], P('gy', None, 'gx'), may hold values from -60 to 60
- diffusivity: float32 [128, 128, 512], P('gy', None, 'gx'), may hold values from 0.5 to 4
- vapour: float32 [128, 128, 512], P('gy', None, 'gx'), may hold values from 0.01 to 0.1
- cos_zenith: float32 [128, 512], P('gy', 'gx'), may hold values from 0.1 to 1
- albedo: float32 [128, 512], P('gy', 'gx'), may hold values from 0.05 to 0.8
- absorption: float32 [128, 112], replicated, may hold values from 0.005 to 1
- solar_weight: float32 [112], replicated, may hold values from 0.002 to 0.02
- day_mask: int32 [512], P(('gx', 'gy')), may hold values from 0 to 1, as said below
Outputs:
- state_next: float32 [128, 128, 512], P('gy', None, 'gx')
- residual: float32 [128, 128, 512], P('gy', None, 'gx')
- net_flux: float32 [128, 128, 512], P('gy', None, 'gx')
The draws below stay inside these ranges and needn't reach their ends.
Inputs may be any that keep to these rules, and one draw needn't show every extreme that they name: `day_mask`: exactly half of the 512 entries are 1, and some device holds only sunlit blocks.
All inputs are finite; a program needn't handle non-finite values.
Results may differ from the reference program's by a relative error of at most 0.00015.
Values sent between devices are 32-bit elements; how exact they have to be, the bound alone decides.
A program may use at most 128 MiB of HBM per device.

```python
import math
import jax
import jax.numpy as jnp
from jax import lax

CX = 128
LEV = 128
G = 112
ITERS = 5
NX = 512
NY = 128
NBLK = 512


def draw_state_prev(key, part):
    latitude = jnp.arange(NY, dtype=jnp.float32)[:, None, None]
    growth = 10.0 ** (latitude / max(NY - 1, 1))
    values = jax.random.normal(key, (NY, LEV, NX), jnp.float32) * growth
    return jnp.clip(values, -60.0, 60.0)


def draw_day_mask(key, part):
    tilt_key, noon_key = jax.random.split(jax.random.fold_in(key, 7))
    blocks_along = NBLK // NY
    tilt = jax.random.randint(tilt_key, (), 0, 2 * blocks_along + 1)
    noon = jax.random.randint(noon_key, (), 0, blocks_along)
    latitude = jnp.arange(NY, dtype=jnp.int32)
    slope = tilt * (2 * latitude + 1 - NY)
    half_width = blocks_along // 2
    offset_rows = jnp.sign(slope) * (jnp.abs(slope) // NY)
    day_width = half_width + jnp.clip(offset_rows, -half_width, half_width)
    longitude = jnp.arange(blocks_along, dtype=jnp.int32)
    distance = (longitude[:, None] - noon) % blocks_along
    sunlit = (distance < day_width[None, :]).astype(jnp.int32)
    return sunlit.reshape(NBLK)


def levels(own_key, extent, cuts, least, largest):
    gain, own = 1.0, jax.random.fold_in(own_key, 6)
    for position, parts in cuts:
        heights = jnp.exp(jax.random.uniform(jax.random.fold_in(own, position), (parts,), jnp.float32, least / len(cuts), largest / len(cuts)))
        gain = gain * jnp.repeat(heights, extent[position] // parts).reshape([-1 if axis == position else 1 for axis in range(len(extent))])
    return gain


def setup_inputs(seed: int = 0) -> dict:
    key_of = jax.random.split(jax.random.key(seed), 9)
    state_prev = draw_state_prev(jax.random.fold_in(key_of[8], 71), 0)
    diffusivity = jnp.clip(jnp.exp(math.log(4.0) - 2.0794415 * jax.random.uniform(key_of[1], (NY, LEV, NX), jnp.float32) ** levels(key_of[1], (NY, LEV, NX), ((0, 8), (2, 4)), -0.2, 0.2)), 0.5, 4.0)
    vapour = jnp.clip(jnp.exp(math.log(0.1) - 2.3025851 * jax.random.uniform(key_of[2], (NY, LEV, NX), jnp.float32) ** levels(key_of[2], (NY, LEV, NX), ((0, 8), (2, 4)), -0.2, 0.2)), 0.01, 0.1)
    cos_zenith = jnp.clip(0.1 + 0.9 * jax.random.uniform(key_of[3], (NY, NX), jnp.float32) ** levels(key_of[3], (NY, NX), ((0, 8), (1, 4)), -0.2, 0.2), 0.1, 1.0)
    albedo = jnp.clip(0.05 + 0.75 * jax.random.uniform(key_of[4], (NY, NX), jnp.float32) ** levels(key_of[4], (NY, NX), ((0, 8), (1, 4)), -0.2, 0.2), 0.05, 0.8)
    absorption = jnp.clip(jnp.exp(jax.random.uniform(key_of[5], (LEV, G), jnp.float32, math.log(0.005), math.log(1.0))), 0.005, 1.0)
    solar_weight = jnp.clip(jnp.exp(jax.random.uniform(key_of[6], (G,), jnp.float32, math.log(0.002), math.log(0.02))), 0.002, 0.02)
    day_mask = draw_day_mask(jax.random.fold_in(key_of[8], 71), 0)
    return dict(state_prev=state_prev, diffusivity=diffusivity, vapour=vapour, cos_zenith=cos_zenith, albedo=albedo, absorption=absorption, solar_weight=solar_weight, day_mask=day_mask)


def neighbours(values):
    widened = jnp.concatenate([values[:, :, -1:], values, values[:, :, :1]], 2)
    extended = jnp.pad(values, ((1, 1), (0, 0), (0, 0)))
    return (widened, extended)

def face_terms(diffusivity):
    widened, extended = neighbours(diffusivity)
    east_face = jnp.sqrt(diffusivity * widened[:, :, 2:])
    west_face = jnp.sqrt(diffusivity * widened[:, :, :-2])
    north_face = jnp.sqrt(diffusivity * extended[2:])
    south_face = jnp.sqrt(diffusivity * extended[:-2])
    level_face = jnp.sqrt(diffusivity[:, 1:] * diffusivity[:, :-1])
    return (east_face, west_face, north_face, south_face, level_face)

def operate(values, conductances):
    east_face, west_face, north_face, south_face, level_face = conductances
    widened, extended = neighbours(values)
    applied = values + east_face * (values - widened[:, :, 2:]) + west_face * (values - widened[:, :, :-2])
    applied = applied + north_face * (values - extended[2:]) + south_face * (values - extended[:-2])
    vertical = level_face * (values[:, 1:] - values[:, :-1])
    padding = jnp.zeros_like(values[:, :1])
    return applied - jnp.concatenate([vertical, padding], 1) + jnp.concatenate([padding, vertical], 1)

def reference(state_prev, diffusivity, vapour, cos_zenith, albedo, absorption, solar_weight, day_mask):
    conductances = face_terms(diffusivity)
    state_next = state_prev
    residual = state_prev - operate(state_prev, conductances)
    direction = residual
    current = jnp.sum(residual * residual)
    for iteration in range(ITERS):
        applied = operate(direction, conductances)
        step_size = current / jnp.sum(direction * applied)
        state_next = state_next + step_size * direction
        residual = residual - step_size * applied
        following = jnp.sum(residual * residual)
        direction = residual + following / current * direction
        current = following
    optical = vapour * (1.0 + 0.5 * jnp.tanh(state_prev))
    absorb32 = absorption.astype(jnp.float32)
    weight32 = solar_weight.astype(jnp.float32)

    def one_row(inputs):
        layer_amount, cosine, surface = inputs
        thickness = absorb32[:, :, None] * layer_amount[:, None, :]
        cumulative = jnp.cumsum(thickness, 0)
        downward = cosine * jnp.exp(-cumulative / cosine)
        upward = surface * downward[-1] * jnp.exp(-1.66 * (cumulative[-1] - cumulative))
        return jnp.einsum('lgc,g->lc', downward - upward, weight32, precision=lax.Precision.HIGHEST)
    fluxes = lax.map(one_row, (optical, cos_zenith, albedo))
    blocks_along = NBLK // NY
    lit_rows = jnp.repeat(day_mask.reshape(blocks_along, NY).T, CX, axis=1).astype(jnp.float32)
    net_flux = fluxes * lit_rows[:, None, :]
    return (state_next, residual, net_flux)
```

```python
import functools
import math

import jax
import jax.numpy as jnp
from jax import lax
from jax.experimental import pallas as pl
from jax.experimental.pallas import tpu as pltpu
from jax.sharding import PartitionSpec as P

ITERS = 5
LANES = 128
SUB = 8
LOG2E = math.log2(math.e)
MESH = pl.DeviceIdType.MESH


def kernel(
    nx, ny,
    state_ref, diff_ref, vapour_ref, cos_ref, albedo_ref, mask_ref, absorb_ref, weight_ref,
    next_ref, residual_ref, net_ref,
    field, east, west, north, level, lon_send, lon_recv,
    wide, down_scale, up_scale, partial, sums, mine, stage_one, half_sum, stage_two,
    lat_ssem, lat_rsem, lon_ssem, lon_rsem, one_ssem, one_rsem, two_ssem, two_rsem,
):
    rows, levels, lanes = state_ref.shape
    gpoints = absorb_ref.shape[0]
    tiles = levels // SUB
    per = lanes // rows
    moments = 2 * ITERS + 1
    ix = lax.axis_index("gx")
    iy = lax.axis_index("gy")
    gx_east, gx_west = lax.rem(ix + 1, nx), lax.rem(ix + nx - 1, nx)
    gy_north, gy_south = lax.rem(iy + 1, ny), lax.rem(iy + ny - 1, ny)
    lane_of = lax.broadcasted_iota(jnp.int32, (SUB, lanes), 1)
    plane_lane = lax.broadcasted_iota(jnp.int32, (levels, lanes), 1)

    barrier = pltpu.get_barrier_semaphore()
    for d in range(1, nx):
        pl.semaphore_signal(
            barrier, inc=1, device_id=(lax.rem(ix + d, nx), iy), device_id_type=MESH
        )
    for d in range(1, ny):
        pl.semaphore_signal(
            barrier, inc=1, device_id=(ix, lax.rem(iy + d, ny)), device_id_type=MESH
        )
    pl.semaphore_wait(barrier, nx + ny - 2)

    def lon_copy(k, side):
        return pltpu.make_async_remote_copy(
            src_ref=lon_send.at[k, side],
            dst_ref=lon_recv.at[k, side],
            send_sem=lon_ssem.at[k, side],
            recv_sem=lon_rsem.at[k, side],
            device_id=(gx_west if side == 0 else gx_east, iy),
            device_id_type=MESH,
        )

    def lat_copy(k, side, source=None):
        if source is not None:
            src = source.at[0 if side == 0 else rows - 1]
        else:
            src = field.at[k, 1 if side == 0 else rows]
        return pltpu.make_async_remote_copy(
            src_ref=src,
            dst_ref=field.at[k, rows + 1 if side == 0 else 0],
            send_sem=lat_ssem.at[k, side],
            recv_sem=lat_rsem.at[k, side],
            device_id=(ix, gy_south if side == 0 else gy_north),
            device_id_type=MESH,
        )

    def pack(k, source):
        groups = tiles // per

        def step(j, packed):
            packed = list(packed)
            for t in range(tiles):
                tile = source[j, t * SUB:(t + 1) * SUB, :]
                target = rows * (t % per) + j
                here = lane_of == target
                for side in range(2):
                    moved = pltpu.roll(tile, lax.rem(target + side, lanes), 1)
                    slot = side * groups + t // per
                    packed[slot] = jnp.where(here, moved, packed[slot])
            return tuple(packed)

        zero = jnp.zeros((SUB, lanes), jnp.float32)
        packed = lax.fori_loop(0, rows, step, (zero,) * (2 * groups))
        for side in range(2):
            for g in range(groups):
                lon_send[k, side, g * SUB:(g + 1) * SUB, :] = packed[side * groups + g]

    def send_halo(k, source):
        for side in range(2):
            lat_copy(k, side, source).start()
        pack(k, field.at[k, 1:rows + 1] if source is None else source)
        for side in range(2):
            lon_copy(k, side).start()

    def wait_halo(k, source=None):
        for side in range(2):
            lat_copy(k, side, source).wait()
            lon_copy(k, side).wait()

    def sides(k, j, plane):
        from_east, from_west = [], []
        for t in range(tiles):
            target = rows * (t % per) + j
            g = t // per
            from_east.append(
                pltpu.roll(lon_recv[k, 0, g * SUB:(g + 1) * SUB, :], lanes - 1 - target, 1)
            )
            from_west.append(
                pltpu.roll(
                    lon_recv[k, 1, g * SUB:(g + 1) * SUB, :], lax.rem(lanes - target, lanes), 1
                )
            )
        from_east = jnp.concatenate(from_east, 0)
        from_west = jnp.concatenate(from_west, 0)
        return (
            jnp.where(plane_lane == lanes - 1, from_east, pltpu.roll(plane, lanes - 1, 1)),
            jnp.where(plane_lane == 0, from_west, pltpu.roll(plane, 1, 1)),
        )

    def flux(k, j):
        plane = field[k, j + 1]
        at_east, at_west = sides(k, j, plane)
        total = east[j] * (plane - at_east) + west[j] * (plane - at_west)
        total = total + north[j + 1] * (plane - field[k, j + 2])
        total = total + north[j] * (plane - field[k, j])
        vertical = level[j] * (pltpu.roll(plane, levels - 1, 0) - plane)
        return total - vertical + pltpu.roll(vertical, 1, 0), plane

    def fold(product):
        return jnp.sum(product.reshape(tiles, SUB, lanes), 0)

    def reduce_copy(r, stage, d):
        buffer = stage_one if stage == 0 else stage_two
        slot = ix if stage == 0 else iy
        ssem = one_ssem if stage == 0 else two_ssem
        rsem = one_rsem if stage == 0 else two_rsem
        peer = (lax.rem(ix + d, nx), iy) if stage == 0 else (ix, lax.rem(iy + d, ny))
        return pltpu.make_async_remote_copy(
            src_ref=(mine if stage == 0 else half_sum).at[r],
            dst_ref=buffer.at[r, slot],
            send_sem=ssem.at[r, d - 1],
            recv_sem=rsem.at[r, d - 1],
            device_id=peer,
            device_id_type=MESH,
        )

    def reduce_start(r, stage):
        source, buffer = (mine, stage_one) if stage == 0 else (half_sum, stage_two)
        n = nx if stage == 0 else ny
        buffer[r, ix if stage == 0 else iy] = source[r]
        for d in range(1, n):
            reduce_copy(r, stage, d).start()

    def reduce_end(r, stage):
        n = nx if stage == 0 else ny
        for d in range(1, n):
            reduce_copy(r, stage, d).wait()
        buffer = stage_one if stage == 0 else stage_two
        total = buffer[r, 0]
        for d in range(1, n):
            total = total + buffer[r, d]
        return total

    def all_lanes(values):
        shift = lanes // 2
        while shift:
            values = values + pltpu.roll(values, shift, 1)
            shift //= 2
        return values

    def radiate(j):
        cosine = cos_ref[pl.ds(j, 1), :]
        optical = vapour_ref[j] * (1.0 + 0.5 * jnp.tanh(state_ref[j]))
        down_scale[...] = optical * (-LOG2E / cosine)
        up_scale[...] = optical * (-1.66 * LOG2E)

        def downward(l, carry):
            carry = carry * jnp.exp2(wide[l] * down_scale[pl.ds(l, 1), :])
            partial[pl.ds(pl.multiple_of(l * SUB, SUB), SUB), :] = jnp.sum(
                carry.reshape(gpoints // SUB, SUB, lanes), 0
            )
            return carry

        carry = lax.fori_loop(0, levels, downward, weight_ref[...] * cosine, unroll=4)
        carry = carry * albedo_ref[pl.ds(j, 1), :]

        def upward(i, carry):
            l = levels - 1 - i
            where = pl.ds(pl.multiple_of(l * SUB, SUB), SUB)
            partial[where, :] = partial[where, :] - jnp.sum(
                carry.reshape(gpoints // SUB, SUB, lanes), 0
            )
            return carry * jnp.exp2(wide[l] * up_scale[pl.ds(l, 1), :])

        lax.fori_loop(0, levels, upward, carry, unroll=4)
        total = partial[pl.ds(0, levels, stride=SUB), :]
        for s in range(1, SUB):
            total = total + partial[pl.ds(s, levels, stride=SUB), :]
        net_ref[j] = total * mask_ref[pl.ds(j, 1), :]

    windows = ITERS + 3

    def window(w):
        @pl.loop(rows * w // windows, rows * (w + 1) // windows)
        def _(j):
            radiate(j)

    send_halo(0, diff_ref)
    send_halo(1, state_ref)

    def spread(j, total):
        field[0, j + 1] = diff_ref[j]
        field[1, j + 1] = state_ref[j]
        return total + fold(diff_ref[j] * diff_ref[j])

    squares = lax.fori_loop(0, rows, spread, jnp.zeros((SUB, lanes), jnp.float32))
    mine[0] = jnp.concatenate([squares, jnp.zeros_like(squares)], 0)
    reduce_start(0, 0)

    absorb = absorb_ref[...]

    @pl.loop(0, levels)
    def _(l):
        column = pltpu.roll(absorb, lax.rem(levels - l, levels), 1)[:, 0:1]
        wide[l] = jnp.broadcast_to(column, (gpoints, lanes))

    window(0)
    half_sum[0] = reduce_end(0, 0)
    reduce_start(0, 1)
    wait_halo(0, diff_ref)
    wait_halo(1, state_ref)

    level_of = lax.broadcasted_iota(jnp.int32, (levels, lanes), 0)

    @pl.loop(0, rows)
    def _(j):
        plane = field[0, j + 1]
        at_east, at_west = sides(0, j, plane)
        east[j] = jnp.sqrt(plane * at_east)
        west[j] = jnp.sqrt(plane * at_west)
        north[j + 1] = jnp.sqrt(plane * field[0, j + 2])
        level[j] = jnp.where(
            level_of == levels - 1, 0.0, jnp.sqrt(plane * pltpu.roll(plane, levels - 1, 0))
        )

    north[0] = jnp.sqrt(field[0, 0] * field[0, 1]) * (iy > 0).astype(jnp.float32)
    north[rows] = north[rows] * (iy < ny - 1).astype(jnp.float32)

    @pl.loop(0, rows)
    def _(j):
        field[2, j + 1] = -flux(1, j)[0]

    send_halo(2, None)
    window(1)
    squares = reduce_end(0, 1)
    count = nx * ny * rows * levels * lanes
    squares = all_lanes(jnp.sum(squares, 0, keepdims=True))
    half = 6.0 * jnp.sqrt(squares * (1.0 / count))
    inverse = 1.0 / half

    zero = jnp.zeros((SUB, lanes), jnp.float32)
    for k in range(ITERS):
        wait_halo(2 + k)

        def advance(j, totals):
            applied, plane = flux(2 + k, j)
            later = applied * inverse - plane
            if k > 0:
                later = 2.0 * later - field[1 + k, j + 1]
            field[3 + k, j + 1] = later
            out = (totals[0] + fold(later * plane), totals[1] + fold(later * later))
            if k == 0:
                out = out + (totals[2] + fold(plane * plane),)
            return out

        totals = lax.fori_loop(0, rows, advance, (zero,) * (3 if k == 0 else 2))
        sums[2 * k + 1] = totals[0]
        sums[2 * k + 2] = totals[1]
        if k == 0:
            sums[0] = totals[2]
        if k < ITERS - 1:
            send_halo(3 + k, None)
            window(2 + k)

    lines = [jnp.sum(sums[m], 0, keepdims=True) for m in range(moments)]
    lines += [jnp.zeros_like(lines[0])] * (2 * SUB - moments)
    mine[1] = jnp.concatenate(lines, 0)
    reduce_start(1, 0)
    window(ITERS + 1)
    half_sum[1] = reduce_end(1, 0)
    reduce_start(1, 1)
    window(ITERS + 2)
    values = all_lanes(reduce_end(1, 1))
    raw = [values[m:m + 1, :] for m in range(moments)]

    mu = [raw[0], raw[1]]
    for k in range(1, ITERS + 1):
        mu.append(2.0 * raw[2 * k] - mu[0])
        if k < ITERS:
            mu.append(2.0 * raw[2 * k + 1] - mu[1])
    gram = [
        [0.5 * (mu[i + j] + mu[abs(i - j)]) for j in range(ITERS + 1)] for i in range(ITERS + 1)
    ]

    def inner(a, b):
        terms = []
        for i in range(len(a)):
            for j in range(len(b)):
                terms.append((a[i] * b[j]) * gram[i][j])
        while len(terms) > 1:
            terms = [
                terms[i] + terms[i + 1] if i + 1 < len(terms) else terms[i]
                for i in range(0, len(terms), 2)
            ]
        return terms[0]

    centre = half + 1.0
    one = jnp.ones_like(half)
    none = jnp.zeros_like(half)
    res, direction, gain = [one], [one], [none] * ITERS
    current = inner(res, res)
    for iteration in range(ITERS):
        image = [centre * c for c in direction] + [none]
        for j, c in enumerate(direction):
            if j == 0:
                image[1] = image[1] + half * c
            else:
                image[j + 1] = image[j + 1] + 0.5 * half * c
                image[j - 1] = image[j - 1] + 0.5 * half * c
        step = current / inner(direction, image)
        for j, c in enumerate(direction):
            gain[j] = gain[j] + step * c
        res = [r - step * q for r, q in zip(res + [none], image)]
        if iteration < ITERS - 1:
            following = inner(res, res)
            ratio = following / current
            direction = [r + ratio * c for r, c in zip(res, direction + [none])]
            current = following

    @pl.loop(0, rows)
    def _(j):
        base = [field[2 + k, j + 1] for k in range(ITERS + 1)]
        iterate, left = state_ref[j], res[0] * base[0]
        for k in range(ITERS):
            iterate = iterate + gain[k] * base[k]
            left = left + res[k + 1] * base[k + 1]
        next_ref[j] = iterate
        residual_ref[j] = left


def body(mesh_shape, state_prev, diffusivity, vapour, cos_zenith, albedo, absorption, solar_weight, day_mask):
    nx, ny = mesh_shape
    rows, levels, lanes = state_prev.shape
    gpoints = absorption.shape[1]
    mask = jnp.broadcast_to(day_mask.astype(jnp.float32)[:, None], (rows, lanes))
    weight = jnp.broadcast_to(solar_weight[:, None], (gpoints, lanes))
    absorb = absorption.T
    f32 = jnp.float32
    out = jax.ShapeDtypeStruct((rows, levels, lanes), f32)
    vmem = pl.BlockSpec(memory_space=pltpu.VMEM)
    kinds = ITERS + 3
    packs = levels // SUB * rows // lanes * SUB
    dma = pltpu.SemaphoreType.DMA
    return pl.pallas_call(
        functools.partial(kernel, nx, ny),
        out_shape=(out, out, out),
        in_specs=[vmem] * 8,
        out_specs=(vmem, vmem, vmem),
        scratch_shapes=[
            pltpu.VMEM((kinds, rows + 2, levels, lanes), f32),
            pltpu.VMEM((rows, levels, lanes), f32),
            pltpu.VMEM((rows, levels, lanes), f32),
            pltpu.VMEM((rows + 1, levels, lanes), f32),
            pltpu.VMEM((rows, levels, lanes), f32),
            pltpu.VMEM((kinds, 2, packs, lanes), f32),
            pltpu.VMEM((kinds, 2, packs, lanes), f32),
            pltpu.VMEM((levels, gpoints, lanes), f32),
            pltpu.VMEM((levels, lanes), f32),
            pltpu.VMEM((levels, lanes), f32),
            pltpu.VMEM((levels * SUB, lanes), f32),
            pltpu.VMEM((2 * ITERS + 1, SUB, lanes), f32),
            pltpu.VMEM((2, 2 * SUB, lanes), f32),
            pltpu.VMEM((2, nx, 2 * SUB, lanes), f32),
            pltpu.VMEM((2, 2 * SUB, lanes), f32),
            pltpu.VMEM((2, ny, 2 * SUB, lanes), f32),
            dma((kinds, 2)), dma((kinds, 2)), dma((kinds, 2)), dma((kinds, 2)),
            dma((2, nx)), dma((2, nx)), dma((2, ny)), dma((2, ny)),
        ],
        compiler_params=pltpu.CompilerParams(
            collective_id=0, has_side_effects=True, vmem_limit_bytes=60 * 1024 * 1024
        ),
    )(state_prev, diffusivity, vapour, cos_zenith, albedo, mask, absorb, weight)


def solution(mesh):
    cells = P("gy", None, "gx")
    columns = P("gy", "gx")
    return jax.shard_map(
        functools.partial(body, (mesh.shape["gx"], mesh.shape["gy"])),
        mesh=mesh,
        in_specs=(cells, cells, cells, columns, columns, P(), P(), P(("gx", "gy"))),
        out_specs=(cells, cells, cells),
        check_vma=False,
    )
```

```python
import functools
import math

import jax
import jax.numpy as jnp
from jax import lax
from jax.experimental import pallas as pl
from jax.experimental.pallas import tpu as pltpu
from jax.sharding import PartitionSpec as P

ITERS = 5
LANES = 128
SUB = 8
LOG2E = math.log2(math.e)
MESH = pl.DeviceIdType.MESH


def kernel(
    nx, ny,
    state_ref, diff_ref, vapour_ref, cos_ref, albedo_ref, mask_ref, absorb_ref, weight_ref,
    next_ref, residual_ref, net_ref,
    field, east, west, north, level, lon_send, lon_recv,
    wide, down_scale, up_scale, partial, sums, mine, stage_one, half_sum, stage_two,
    lat_ssem, lat_rsem, lon_ssem, lon_rsem, one_ssem, one_rsem, two_ssem, two_rsem,
):
    rows, levels, lanes = state_ref.shape
    gpoints = absorb_ref.shape[0]
    tiles = levels // SUB
    per = lanes // rows
    moments = 2 * ITERS + 1
    ix = lax.axis_index("gx")
    iy = lax.axis_index("gy")
    gx_east, gx_west = lax.rem(ix + 1, nx), lax.rem(ix + nx - 1, nx)
    gy_north, gy_south = lax.rem(iy + 1, ny), lax.rem(iy + ny - 1, ny)
    lane_of = lax.broadcasted_iota(jnp.int32, (SUB, lanes), 1)
    plane_lane = lax.broadcasted_iota(jnp.int32, (levels, lanes), 1)

    barrier = pltpu.get_barrier_semaphore()
    for d in range(1, nx):
        pl.semaphore_signal(
            barrier, inc=1, device_id=(lax.rem(ix + d, nx), iy), device_id_type=MESH
        )
    for d in range(1, ny):
        pl.semaphore_signal(
            barrier, inc=1, device_id=(ix, lax.rem(iy + d, ny)), device_id_type=MESH
        )
    pl.semaphore_wait(barrier, nx + ny - 2)

    def lon_copy(k, side):
        return pltpu.make_async_remote_copy(
            src_ref=lon_send.at[k, side],
            dst_ref=lon_recv.at[k, side],
            send_sem=lon_ssem.at[k, side],
            recv_sem=lon_rsem.at[k, side],
            device_id=(gx_west if side == 0 else gx_east, iy),
            device_id_type=MESH,
        )

    def lat_copy(k, side, source=None):
        if source is not None:
            src = source.at[0 if side == 0 else rows - 1]
        else:
            src = field.at[k, 1 if side == 0 else rows]
        return pltpu.make_async_remote_copy(
            src_ref=src,
            dst_ref=field.at[k, rows + 1 if side == 0 else 0],
            send_sem=lat_ssem.at[k, side],
            recv_sem=lat_rsem.at[k, side],
            device_id=(ix, gy_south if side == 0 else gy_north),
            device_id_type=MESH,
        )

    def pack(k, source):
        groups = tiles // per

        def step(j, packed):
            packed = list(packed)
            for t in range(tiles):
                tile = source[j, t * SUB:(t + 1) * SUB, :]
                target = rows * (t % per) + j
                here = lane_of == target
                for side in range(2):
                    moved = pltpu.roll(tile, lax.rem(target + side, lanes), 1)
                    slot = side * groups + t // per
                    packed[slot] = jnp.where(here, moved, packed[slot])
            return tuple(packed)

        zero = jnp.zeros((SUB, lanes), jnp.float32)
        packed = lax.fori_loop(0, rows, step, (zero,) * (2 * groups))
        for side in range(2):
            for g in range(groups):
                lon_send[k, side, g * SUB:(g + 1) * SUB, :] = packed[side * groups + g]

    def send_halo(k, source):
        for side in range(2):
            lat_copy(k, side, source).start()
        pack(k, field.at[k, 1:rows + 1] if source is None else source)
        for side in range(2):
            lon_copy(k, side).start()

    def wait_halo(k, source=None):
        for side in range(2):
            lat_copy(k, side, source).wait()
            lon_copy(k, side).wait()

    def sides(k, j, plane):
        from_east, from_west = [], []
        for t in range(tiles):
            target = rows * (t % per) + j
            g = t // per
            from_east.append(
                pltpu.roll(lon_recv[k, 0, g * SUB:(g + 1) * SUB, :], lanes - 1 - target, 1)
            )
            from_west.append(
                pltpu.roll(
                    lon_recv[k, 1, g * SUB:(g + 1) * SUB, :], lax.rem(lanes - target, lanes), 1
                )
            )
        from_east = jnp.concatenate(from_east, 0)
        from_west = jnp.concatenate(from_west, 0)
        return (
            jnp.where(plane_lane == lanes - 1, from_east, pltpu.roll(plane, lanes - 1, 1)),
            jnp.where(plane_lane == 0, from_west, pltpu.roll(plane, 1, 1)),
        )

    def flux(k, j):
        plane = field[k, j + 1]
        at_east, at_west = sides(k, j, plane)
        total = east[j] * (plane - at_east) + west[j] * (plane - at_west)
        total = total + north[j + 1] * (plane - field[k, j + 2])
        total = total + north[j] * (plane - field[k, j])
        vertical = level[j] * (pltpu.roll(plane, levels - 1, 0) - plane)
        return total - vertical + pltpu.roll(vertical, 1, 0), plane

    def fold(product):
        return jnp.sum(product.reshape(tiles, SUB, lanes), 0)

    def reduce_copy(r, stage, d):
        buffer = stage_one if stage == 0 else stage_two
        slot = ix if stage == 0 else iy
        ssem = one_ssem if stage == 0 else two_ssem
        rsem = one_rsem if stage == 0 else two_rsem
        peer = (lax.rem(ix + d, nx), iy) if stage == 0 else (ix, lax.rem(iy + d, ny))
        return pltpu.make_async_remote_copy(
            src_ref=(mine if stage == 0 else half_sum).at[r],
            dst_ref=buffer.at[r, slot],
            send_sem=ssem.at[r, d - 1],
            recv_sem=rsem.at[r, d - 1],
            device_id=peer,
            device_id_type=MESH,
        )

    def reduce_start(r, stage):
        source, buffer = (mine, stage_one) if stage == 0 else (half_sum, stage_two)
        n = nx if stage == 0 else ny
        buffer[r, ix if stage == 0 else iy] = source[r]
        for d in range(1, n):
            reduce_copy(r, stage, d).start()

    def reduce_end(r, stage):
        n = nx if stage == 0 else ny
        for d in range(1, n):
            reduce_copy(r, stage, d).wait()
        buffer = stage_one if stage == 0 else stage_two
        total = buffer[r, 0]
        for d in range(1, n):
            total = total + buffer[r, d]
        return total

    def all_lanes(values):
        shift = lanes // 2
        while shift:
            values = values + pltpu.roll(values, shift, 1)
            shift //= 2
        return values

    def radiate(j):
        cosine = cos_ref[pl.ds(j, 1), :]
        optical = vapour_ref[j] * (1.0 + 0.5 * jnp.tanh(state_ref[j]))
        down_scale[...] = optical * (-LOG2E / cosine)
        up_scale[...] = optical * (-1.66 * LOG2E)

        def downward(l, carry):
            carry = carry * jnp.exp2(wide[l] * down_scale[pl.ds(l, 1), :])
            partial[pl.ds(pl.multiple_of(l * SUB, SUB), SUB), :] = jnp.sum(
                carry.reshape(gpoints // SUB, SUB, lanes), 0
            )
            return carry

        carry = lax.fori_loop(0, levels, downward, weight_ref[...] * cosine, unroll=8)
        carry = carry * albedo_ref[pl.ds(j, 1), :]

        def upward(i, carry):
            l = levels - 1 - i
            where = pl.ds(pl.multiple_of(l * SUB, SUB), SUB)
            partial[where, :] = partial[where, :] - jnp.sum(
                carry.reshape(gpoints // SUB, SUB, lanes), 0
            )
            return carry * jnp.exp2(wide[l] * up_scale[pl.ds(l, 1), :])

        lax.fori_loop(0, levels, upward, carry, unroll=8)
        total = partial[pl.ds(0, levels, stride=SUB), :]
        for s in range(1, SUB):
            total = total + partial[pl.ds(s, levels, stride=SUB), :]
        net_ref[j] = total * mask_ref[pl.ds(j, 1), :]

    windows = ITERS + 3

    def window(w):
        @pl.loop(rows * w // windows, rows * (w + 1) // windows)
        def _(j):
            radiate(j)

    send_halo(0, diff_ref)
    send_halo(1, state_ref)

    def spread(j, total):
        field[0, j + 1] = diff_ref[j]
        field[1, j + 1] = state_ref[j]
        square = diff_ref[j] * diff_ref[j]
        return total + fold(square * square * square)

    squares = lax.fori_loop(0, rows, spread, jnp.zeros((SUB, lanes), jnp.float32))
    mine[0] = jnp.concatenate([squares, jnp.zeros_like(squares)], 0)
    reduce_start(0, 0)

    absorb = absorb_ref[...]

    @pl.loop(0, levels)
    def _(l):
        column = pltpu.roll(absorb, lax.rem(levels - l, levels), 1)[:, 0:1]
        wide[l] = jnp.broadcast_to(column, (gpoints, lanes))

    window(0)
    half_sum[0] = reduce_end(0, 0)
    reduce_start(0, 1)
    wait_halo(0, diff_ref)
    wait_halo(1, state_ref)

    level_of = lax.broadcasted_iota(jnp.int32, (levels, lanes), 0)

    @pl.loop(0, rows)
    def _(j):
        plane = field[0, j + 1]
        at_east, at_west = sides(0, j, plane)
        east[j] = jnp.sqrt(plane * at_east)
        west[j] = jnp.sqrt(plane * at_west)
        north[j + 1] = jnp.sqrt(plane * field[0, j + 2])
        level[j] = jnp.where(
            level_of == levels - 1, 0.0, jnp.sqrt(plane * pltpu.roll(plane, levels - 1, 0))
        )

    north[0] = jnp.sqrt(field[0, 0] * field[0, 1]) * (iy > 0).astype(jnp.float32)
    north[rows] = north[rows] * (iy < ny - 1).astype(jnp.float32)

    @pl.loop(0, rows)
    def _(j):
        field[2, j + 1] = -flux(1, j)[0]

    send_halo(2, None)
    window(1)
    squares = reduce_end(0, 1)
    count = nx * ny * rows * levels * lanes
    squares = all_lanes(jnp.sum(squares, 0, keepdims=True))
    half = 6.0 * jnp.exp(jnp.log(squares * (1.0 / count)) * (1.0 / 6.0))
    inverse = 1.0 / half

    zero = jnp.zeros((SUB, lanes), jnp.float32)
    for k in range(ITERS):
        wait_halo(2 + k)

        def advance(j, totals):
            applied, plane = flux(2 + k, j)
            later = applied * inverse - plane
            if k > 0:
                later = 2.0 * later - field[1 + k, j + 1]
            field[3 + k, j + 1] = later
            out = (totals[0] + fold(later * plane), totals[1] + fold(later * later))
            if k == 0:
                out = out + (totals[2] + fold(plane * plane),)
            return out

        totals = lax.fori_loop(0, rows, advance, (zero,) * (3 if k == 0 else 2))
        sums[2 * k + 1] = totals[0]
        sums[2 * k + 2] = totals[1]
        if k == 0:
            sums[0] = totals[2]
        if k < ITERS - 1:
            send_halo(3 + k, None)
            window(2 + k)

    lines = [jnp.sum(sums[m], 0, keepdims=True) for m in range(moments)]
    lines += [jnp.zeros_like(lines[0])] * (2 * SUB - moments)
    mine[1] = jnp.concatenate(lines, 0)
    reduce_start(1, 0)
    window(ITERS + 1)
    half_sum[1] = reduce_end(1, 0)
    reduce_start(1, 1)
    window(ITERS + 2)
    values = all_lanes(reduce_end(1, 1))
    raw = [values[m:m + 1, :] for m in range(moments)]

    mu = [raw[0], raw[1]]
    for k in range(1, ITERS + 1):
        mu.append(2.0 * raw[2 * k] - mu[0])
        if k < ITERS:
            mu.append(2.0 * raw[2 * k + 1] - mu[1])
    gram = [
        [0.5 * (mu[i + j] + mu[abs(i - j)]) for j in range(ITERS + 1)] for i in range(ITERS + 1)
    ]

    def inner(a, b):
        terms = []
        for i in range(len(a)):
            for j in range(len(b)):
                terms.append((a[i] * b[j]) * gram[i][j])
        while len(terms) > 1:
            terms = [
                terms[i] + terms[i + 1] if i + 1 < len(terms) else terms[i]
                for i in range(0, len(terms), 2)
            ]
        return terms[0]

    centre = half + 1.0
    one = jnp.ones_like(half)
    none = jnp.zeros_like(half)
    res, direction, gain = [one], [one], [none] * ITERS
    current = inner(res, res)
    for iteration in range(ITERS):
        image = [centre * c for c in direction] + [none]
        for j, c in enumerate(direction):
            if j == 0:
                image[1] = image[1] + half * c
            else:
                image[j + 1] = image[j + 1] + 0.5 * half * c
                image[j - 1] = image[j - 1] + 0.5 * half * c
        step = current / inner(direction, image)
        for j, c in enumerate(direction):
            gain[j] = gain[j] + step * c
        res = [r - step * q for r, q in zip(res + [none], image)]
        if iteration < ITERS - 1:
            following = inner(res, res)
            ratio = following / current
            direction = [r + ratio * c for r, c in zip(res, direction + [none])]
            current = following

    @pl.loop(0, rows)
    def _(j):
        base = [field[2 + k, j + 1] for k in range(ITERS + 1)]
        iterate, left = state_ref[j], res[0] * base[0]
        for k in range(ITERS):
            iterate = iterate + gain[k] * base[k]
            left = left + res[k + 1] * base[k + 1]
        next_ref[j] = iterate
        residual_ref[j] = left


def body(mesh_shape, state_prev, diffusivity, vapour, cos_zenith, albedo, absorption, solar_weight, day_mask):
    nx, ny = mesh_shape
    rows, levels, lanes = state_prev.shape
    gpoints = absorption.shape[1]
    mask = jnp.broadcast_to(day_mask.astype(jnp.float32)[:, None], (rows, lanes))
    weight = jnp.broadcast_to(solar_weight[:, None], (gpoints, lanes))
    absorb = absorption.T
    f32 = jnp.float32
    out = jax.ShapeDtypeStruct((rows, levels, lanes), f32)
    vmem = pl.BlockSpec(memory_space=pltpu.VMEM)
    kinds = ITERS + 3
    packs = levels // SUB * rows // lanes * SUB
    dma = pltpu.SemaphoreType.DMA
    return pl.pallas_call(
        functools.partial(kernel, nx, ny),
        out_shape=(out, out, out),
        in_specs=[vmem] * 8,
        out_specs=(vmem, vmem, vmem),
        scratch_shapes=[
            pltpu.VMEM((kinds, rows + 2, levels, lanes), f32),
            pltpu.VMEM((rows, levels, lanes), f32),
            pltpu.VMEM((rows, levels, lanes), f32),
            pltpu.VMEM((rows + 1, levels, lanes), f32),
            pltpu.VMEM((rows, levels, lanes), f32),
            pltpu.VMEM((kinds, 2, packs, lanes), f32),
            pltpu.VMEM((kinds, 2, packs, lanes), f32),
            pltpu.VMEM((levels, gpoints, lanes), f32),
            pltpu.VMEM((levels, lanes), f32),
            pltpu.VMEM((levels, lanes), f32),
            pltpu.VMEM((levels * SUB, lanes), f32),
            pltpu.VMEM((2 * ITERS + 1, SUB, lanes), f32),
            pltpu.VMEM((2, 2 * SUB, lanes), f32),
            pltpu.VMEM((2, nx, 2 * SUB, lanes), f32),
            pltpu.VMEM((2, 2 * SUB, lanes), f32),
            pltpu.VMEM((2, ny, 2 * SUB, lanes), f32),
            dma((kinds, 2)), dma((kinds, 2)), dma((kinds, 2)), dma((kinds, 2)),
            dma((2, nx)), dma((2, nx)), dma((2, ny)), dma((2, ny)),
        ],
        compiler_params=pltpu.CompilerParams(
            collective_id=0, has_side_effects=True, vmem_limit_bytes=60 * 1024 * 1024
        ),
    )(state_prev, diffusivity, vapour, cos_zenith, albedo, mask, absorb, weight)


def solution(mesh):
    cells = P("gy", None, "gx")
    columns = P("gy", "gx")
    return jax.shard_map(
        functools.partial(body, (mesh.shape["gx"], mesh.shape["gy"])),
        mesh=mesh,
        in_specs=(cells, cells, cells, columns, columns, P(), P(), P(("gx", "gy"))),
        out_specs=(cells, cells, cells),
        check_vma=False,
    )
```
